32 devices in a mesh: zero: 16 (over z, y, core), width: 2 (over x).
Axes of the slice: x: 2, y: 2, z: 4, core: 2. Of those that a mesh axis runs over, the one named last changes fastest.
Arguments:
- slopes_in: float32 [128, 128, 4096], P(None, 'zero', 'width'), may hold values from -6 to 6
- moments_in: float32 [128, 128, 4096], P(None, 'zero', 'width'), may hold values from -6 to 6
- weights_in: float32 [128, 128, 4096], P(None, 'zero', 'width'), may hold values from -0.1875 to 0.1875
Outputs:
- new_weights: float32 [128, 128, 4096], P(None, 'zero', 'width')
- new_momentum: float32 [128, 128, 4096], P(None, 'zero', 'width')
The draws below stay inside these ranges and needn't reach their ends.
All inputs are finite; a program needn't handle non-finite values.
Results may differ from the reference program's by a relative error of at most 0.0001.
Values sent between devices are 32-bit elements; how exact they have to be, the bound alone decides.
A program may use at most 128 MiB of HBM per device.

```python
import jax
import jax.numpy as jnp
from jax import lax

SIDE = 128
WIDE = 4096
MATS = 128
ITERS = 3


def level_of(stream_key, shape, pieces, smallest, high):
    def one(dim, parts):
        draws = jax.random.uniform(jax.random.fold_in(jax.random.fold_in(stream_key, 6), dim), (parts,), jnp.float32, smallest / len(pieces), high / len(pieces))
        return jnp.repeat(jnp.exp(draws), shape[dim] // parts).reshape((-1,) + (1,) * (len(shape) - dim - 1))

    factor_of = one(*pieces[0])
    for cut in pieces[1:]:
        factor_of = factor_of * one(*cut)
    return factor_of


def normal_values(rng, extent, spread, limit, cuts=(), held_as=jnp.bfloat16):
    values = jax.random.normal(rng, extent, jnp.float32) * spread
    if len(cuts) > 0:
        values = level_of(rng, extent, cuts, -0.22, 0.18) * values
    return jnp.clip(values, min=-limit, max=limit).astype(held_as)


def setup_inputs(seed: int = 0) -> dict:
    keys = jax.random.split(jax.random.key(seed), 4)
    slopes_in = normal_values(keys[0], (MATS, SIDE, WIDE), 1.0, 6.0, ((1, 16), (2, 2)), jnp.float32)
    moments_in = normal_values(keys[1], (MATS, SIDE, WIDE), 1.0, 6.0, ((1, 16), (2, 2)), jnp.float32)
    weights_in = normal_values(keys[2], (MATS, SIDE, WIDE), 0.03, 0.1875, ((1, 16), (2, 2)), jnp.float32)
    return dict(slopes_in=slopes_in, moments_in=moments_in, weights_in=weights_in)


hold_rate = 0.8
learn_rate = 0.8
decay_rate = 0.1

def reference(slopes_in, moments_in, weights_in):
    new_momentum = hold_rate * moments_in + slopes_in
    direction = hold_rate * new_momentum + slopes_in

    def orthogonal_one(stack):
        iterate = stack[None]
        iterate = iterate * lax.rsqrt(lax.optimization_barrier(jnp.sum(iterate * iterate, axis=(1, 2), keepdims=True)) + 1e-06)
        for step in range(ITERS):
            gram = jnp.einsum('mik,mjk->mij', iterate, iterate, precision=lax.Precision.HIGHEST)
            mixed = -4.775 * gram + 2.0315 * jnp.einsum('mij,mjk->mik', gram, gram, precision=lax.Precision.HIGHEST)
            iterate = 3.4445 * iterate + jnp.einsum('mij,mjk->mik', mixed, iterate, precision=lax.Precision.HIGHEST)
        return iterate[0]
    iterate = lax.map(orthogonal_one, direction)
    new_weights = (1.0 - learn_rate * decay_rate) * weights_in - learn_rate * iterate
    return (new_weights, new_momentum)
```

```python
import functools

import jax
import jax.numpy as jnp
from jax import lax
from jax.experimental import pallas as pl
from jax.experimental.pallas import tpu as pltpu
from jax.sharding import PartitionSpec as P

ITERS = 3
MESH = pl.DeviceIdType.MESH

hold_rate = 0.8
learn_rate = 0.8
decay_rate = 0.1


def dot(a, b):
    return jnp.dot(a, b, precision=lax.Precision.HIGHEST, preferred_element_type=jnp.float32)


def kernel(nz, nw, sent, back, held, made, gram, heard, fwd_send, fwd_recv, gram_send, gram_recv, ret_send, ret_recv, own_sem):
    me = lax.axis_index("zero")
    side = lax.axis_index("width")
    mats, rows, cols = sent.shape
    mine = mats // nz
    total_rows = nz * rows

    barrier = pltpu.get_barrier_semaphore()

    def greet_zero(k, c):
        pl.semaphore_signal(barrier, inc=1, device_id=(lax.rem(me + k, nz), side), device_id_type=MESH)
        return c

    def greet_width(k, c):
        pl.semaphore_signal(barrier, inc=1, device_id=(me, lax.rem(side + k, nw)), device_id_type=MESH)
        return c

    lax.fori_loop(1, nz, greet_zero, 0)
    lax.fori_loop(1, nw, greet_width, 0)
    pl.semaphore_wait(barrier, nz - 1 + nw - 1)

    def forward(j, c):
        pltpu.make_async_copy(sent.at[me * mine + j], held.at[j, me], fwd_recv.at[j]).start()

        def one(k, c):
            to = lax.rem(me + k, nz)
            pltpu.make_async_remote_copy(
                src_ref=sent.at[to * mine + j],
                dst_ref=held.at[j, me],
                send_sem=fwd_send,
                recv_sem=fwd_recv.at[j],
                device_id=(to, side),
                device_id_type=MESH,
            ).start()
            return c

        return lax.fori_loop(1, nz, one, c)

    lax.fori_loop(0, mine, forward, 0)

    def gram_of(j):
        pltpu.make_async_copy(held.at[j], held.at[j], fwd_recv.at[j]).wait()
        x = held[j].reshape(total_rows, cols)
        gram[j] = lax.dot_general(
            x, x, (((1,), (1,)), ((), ())),
            precision=lax.Precision.HIGHEST, preferred_element_type=jnp.float32,
        )

        def one(k, c):
            to = lax.rem(side + k, nw)
            pltpu.make_async_remote_copy(
                src_ref=gram.at[j],
                dst_ref=heard.at[j, k - 1],
                send_sem=gram_send,
                recv_sem=gram_recv.at[j],
                device_id=(me, to),
                device_id_type=MESH,
            ).start()
            return c

        lax.fori_loop(1, nw, one, 0)

    def finish(j):
        pltpu.make_async_copy(heard.at[j], heard.at[j], gram_recv.at[j]).wait()
        full = gram[j] + jnp.sum(heard[j], axis=0)
        at_diag = lax.broadcasted_iota(jnp.int32, full.shape, 0) == lax.broadcasted_iota(jnp.int32, full.shape, 1)
        squares = jnp.sum(jnp.sum(jnp.where(at_diag, full, 0.0), axis=1, keepdims=True), axis=0, keepdims=True)
        scale = lax.rsqrt(squares + 1e-06)
        a = full * scale * scale
        eye = jnp.where(at_diag, 3.4445, 0.0)
        mix = None
        for step in range(ITERS):
            m = eye - 4.775 * a + 2.0315 * dot(a, a)
            if step < ITERS - 1:
                a = dot(dot(m, a), m)
            mix = m if mix is None else dot(m, mix)
        mix = mix * scale
        y = dot(mix, held[j].reshape(total_rows, cols))
        made[j] = y.reshape(nz, rows, cols)
        pltpu.make_async_copy(made.at[j, me], back.at[me * mine + j], own_sem).start()

        def one(k, c):
            to = lax.rem(me + k, nz)
            pltpu.make_async_remote_copy(
                src_ref=made.at[j, to],
                dst_ref=back.at[me * mine + j],
                send_sem=ret_send,
                recv_sem=ret_recv,
                device_id=(to, side),
                device_id_type=MESH,
            ).start()
            return c

        lax.fori_loop(1, nz, one, 0)

    gram_of(0)

    def stage(j, c):
        gram_of(j)
        finish(j - 1)
        return c

    lax.fori_loop(1, mine, stage, 0)
    finish(mine - 1)

    others = pl.ds(0, (nz - 1) * mine)
    own = pl.ds(0, mine)
    pltpu.make_async_copy(sent.at[others], sent.at[others], fwd_send).wait()
    pltpu.make_async_copy(heard, heard, gram_send).wait()
    pltpu.make_async_copy(back.at[others], back.at[others], ret_send).wait()
    pltpu.make_async_copy(back.at[others], back.at[others], ret_recv).wait()
    pltpu.make_async_copy(back.at[own], back.at[own], own_sem).wait()


def orthogonal(nz, nw, direction):
    mats, rows, cols = direction.shape
    mine = mats // nz
    n = nz * rows
    return pl.pallas_call(
        functools.partial(kernel, nz, nw),
        out_shape=jax.ShapeDtypeStruct(direction.shape, jnp.float32),
        in_specs=[pl.BlockSpec(memory_space=pltpu.HBM)],
        out_specs=pl.BlockSpec(memory_space=pltpu.HBM),
        scratch_shapes=[
            pltpu.VMEM((mine, nz, rows, cols), jnp.float32),
            pltpu.VMEM((mine, nz, rows, cols), jnp.float32),
            pltpu.VMEM((mine, n, n), jnp.float32),
            pltpu.VMEM((mine, nw - 1, n, n), jnp.float32),
            pltpu.SemaphoreType.DMA,
            pltpu.SemaphoreType.DMA((mine,)),
            pltpu.SemaphoreType.DMA,
            pltpu.SemaphoreType.DMA((mine,)),
            pltpu.SemaphoreType.DMA,
            pltpu.SemaphoreType.DMA,
            pltpu.SemaphoreType.DMA,
        ],
        compiler_params=pltpu.CompilerParams(
            collective_id=0, has_side_effects=True, vmem_limit_bytes=48 * 1024 * 1024
        ),
        name="orthogonal",
    )(direction)


def body(nz, nw, slopes_in, moments_in, weights_in):
    new_momentum = hold_rate * moments_in + slopes_in
    direction = hold_rate * new_momentum + slopes_in
    back = orthogonal(nz, nw, direction)
    new_weights = (1.0 - learn_rate * decay_rate) * weights_in - learn_rate * back
    return (new_weights, new_momentum)


def solution(mesh):
    spec = P(None, "zero", "width")
    run = functools.partial(body, mesh.shape["zero"], mesh.shape["width"])
    return jax.shard_map(run, mesh=mesh, in_specs=(spec,) * 3, out_specs=(spec,) * 2, check_vma=False)
```

```python
import functools

import jax
import jax.numpy as jnp
from jax import lax
from jax.experimental import pallas as pl
from jax.experimental.pallas import tpu as pltpu
from jax.sharding import PartitionSpec as P

ITERS = 3
MESH = pl.DeviceIdType.MESH

hold_rate = 0.8
learn_rate = 0.8
decay_rate = 0.1


def dot(a, b):
    return jnp.dot(a, b, precision=lax.Precision.HIGHEST, preferred_element_type=jnp.float32)


def kernel(
    nz, nw, sent, weights, new_weights, held, made, back, old, gram, heard,
    fwd_send, fwd_recv, gram_send, gram_recv, ret_send, ret_recv, old_sem, new_sem,
):
    me = lax.axis_index("zero")
    side = lax.axis_index("width")
    mats, rows, cols = sent.shape
    mine = mats // nz
    total_rows = nz * rows

    barrier = pltpu.get_barrier_semaphore()

    def greet_zero(k, c):
        pl.semaphore_signal(barrier, inc=1, device_id=(lax.rem(me + k, nz), side), device_id_type=MESH)
        return c

    def greet_width(k, c):
        pl.semaphore_signal(barrier, inc=1, device_id=(me, lax.rem(side + k, nw)), device_id_type=MESH)
        return c

    lax.fori_loop(1, nz, greet_zero, 0)
    lax.fori_loop(1, nw, greet_width, 0)
    pl.semaphore_wait(barrier, nz - 1 + nw - 1)

    def forward(j, c):
        pltpu.make_async_copy(sent.at[me * mine + j], held.at[j, me], fwd_recv.at[j]).start()

        def one(k, c):
            to = lax.rem(me + k, nz)
            pltpu.make_async_remote_copy(
                src_ref=sent.at[to * mine + j],
                dst_ref=held.at[j, me],
                send_sem=fwd_send,
                recv_sem=fwd_recv.at[j],
                device_id=(to, side),
                device_id_type=MESH,
            ).start()
            return c

        return lax.fori_loop(1, nz, one, c)

    lax.fori_loop(0, mine, forward, 0)
    pltpu.make_async_copy(weights, old, old_sem).start()

    def gram_of(j):
        pltpu.make_async_copy(held.at[j], held.at[j], fwd_recv.at[j]).wait()
        x = held[j].reshape(total_rows, cols)
        gram[j] = lax.dot_general(
            x, x, (((1,), (1,)), ((), ())),
            precision=lax.Precision.HIGHEST, preferred_element_type=jnp.float32,
        )

        def one(k, c):
            to = lax.rem(side + k, nw)
            pltpu.make_async_remote_copy(
                src_ref=gram.at[j],
                dst_ref=heard.at[j, k - 1],
                send_sem=gram_send,
                recv_sem=gram_recv.at[j],
                device_id=(me, to),
                device_id_type=MESH,
            ).start()
            return c

        lax.fori_loop(1, nw, one, 0)

    def finish(j):
        pltpu.make_async_copy(heard.at[j], heard.at[j], gram_recv.at[j]).wait()
        full = gram[j] + jnp.sum(heard[j], axis=0)
        at_diag = lax.broadcasted_iota(jnp.int32, full.shape, 0) == lax.broadcasted_iota(jnp.int32, full.shape, 1)
        squares = jnp.sum(jnp.sum(jnp.where(at_diag, full, 0.0), axis=1, keepdims=True), axis=0, keepdims=True)
        scale = lax.rsqrt(squares + 1e-06)
        a = full * scale * scale
        eye = jnp.where(at_diag, 3.4445, 0.0)
        mix = None
        for step in range(ITERS):
            m = eye - 4.775 * a + 2.0315 * dot(a, a)
            if step < ITERS - 1:
                a = dot(dot(m, a), m)
            mix = m if mix is None else dot(m, mix)
        mix = mix * scale
        y = dot(mix, held[j].reshape(total_rows, cols))
        made[j] = y.reshape(nz, rows, cols)

        def one(k, c):
            to = lax.rem(me + k, nz)
            pltpu.make_async_remote_copy(
                src_ref=made.at[j, to],
                dst_ref=back.at[me * mine + j],
                send_sem=ret_send,
                recv_sem=ret_recv.at[j],
                device_id=(to, side),
                device_id_type=MESH,
            ).start()
            return c

        lax.fori_loop(1, nz, one, 0)
        back[me * mine + j] = made[j, me]

    gram_of(0)

    def stage(j, c):
        gram_of(j)
        finish(j - 1)
        return c

    lax.fori_loop(1, mine, stage, 0)
    finish(mine - 1)

    pltpu.make_async_copy(weights, old, old_sem).wait()

    def update(j, c):
        came = back.at[pl.ds(0, nz - 1)]
        pltpu.make_async_copy(came, came, ret_recv.at[j]).wait()

        def one(k, c):
            at = k * mine + j
            back[at] = (1.0 - learn_rate * decay_rate) * old[at] - learn_rate * back[at]
            return c

        def leave(k, c):
            at = k * mine + j
            pltpu.make_async_copy(back.at[at], new_weights.at[at], new_sem).start()
            return c

        lax.fori_loop(0, nz, one, 0)
        return lax.fori_loop(0, nz, leave, c)

    lax.fori_loop(0, mine, update, 0)

    others = pl.ds(0, (nz - 1) * mine)
    pltpu.make_async_copy(sent.at[others], sent.at[others], fwd_send).wait()
    pltpu.make_async_copy(heard, heard, gram_send).wait()
    pltpu.make_async_copy(back.at[others], back.at[others], ret_send).wait()
    pltpu.make_async_copy(back, new_weights, new_sem).wait()


def stepped(nz, nw, direction, weights):
    mats, rows, cols = direction.shape
    mine = mats // nz
    n = nz * rows
    return pl.pallas_call(
        functools.partial(kernel, nz, nw),
        out_shape=jax.ShapeDtypeStruct(direction.shape, jnp.float32),
        in_specs=[pl.BlockSpec(memory_space=pl.ANY), pl.BlockSpec(memory_space=pltpu.HBM)],
        out_specs=pl.BlockSpec(memory_space=pltpu.HBM),
        scratch_shapes=[
            pltpu.VMEM((mine, nz, rows, cols), jnp.float32),
            pltpu.VMEM((mine, nz, rows, cols), jnp.float32),
            pltpu.VMEM(direction.shape, jnp.float32),
            pltpu.VMEM(direction.shape, jnp.float32),
            pltpu.VMEM((mine, n, n), jnp.float32),
            pltpu.VMEM((mine, nw - 1, n, n), jnp.float32),
            pltpu.SemaphoreType.DMA,
            pltpu.SemaphoreType.DMA((mine,)),
            pltpu.SemaphoreType.DMA,
            pltpu.SemaphoreType.DMA((mine,)),
            pltpu.SemaphoreType.DMA,
            pltpu.SemaphoreType.DMA((mine,)),
            pltpu.SemaphoreType.DMA,
            pltpu.SemaphoreType.DMA,
        ],
        compiler_params=pltpu.CompilerParams(
            collective_id=0, has_side_effects=True, vmem_limit_bytes=38 * 1024 * 1024
        ),
        name="stepped",
    )(direction, weights)


def body(nz, nw, slopes_in, moments_in, weights_in):
    new_momentum = hold_rate * moments_in + slopes_in
    direction = hold_rate * new_momentum + slopes_in
    new_weights = stepped(nz, nw, direction, weights_in)
    return (new_weights, new_momentum)


def solution(mesh):
    spec = P(None, "zero", "width")
    run = functools.partial(body, mesh.shape["zero"], mesh.shape["width"])
    return jax.shard_map(run, mesh=mesh, in_specs=(spec,) * 3, out_specs=(spec,) * 2, check_vma=False)
```
